128 devices in a mesh: rep: 2 (over y_lo), own: 64 (over x, z, y_hi, core).
Axes of the slice: x: 4, y: 4 (y_hi: 2, y_lo: 2; y = y_hi * 2 + y_lo), z: 4, core: 2. Of those that a mesh axis runs over, the one named last changes fastest.
Arguments:
- values: float32 [1048576, 128], P(('rep', 'own')), may hold values from -0.8 to 0.8
- key_ids: int32 [1048576], P(('rep', 'own')), may hold values from 0 to 262143, as said below
- heavy_ids: int32 [2048], replicated, may hold values from 0 to 262143, as said below
- block_offsets: int32 [128, 64], P(('rep', 'own')), may hold values from 0 to 8191, as said below
- block_counts: int32 [128, 64], P(('rep', 'own')), may hold values from 8 to 64, as said below
Outputs:
- light_sums: float32 [262144, 128], P('own')
- heavy_sums: float32 [2048, 128], P('own')
The draws below stay inside these ranges and needn't reach their ends.
Inputs may be any that keep to these rules, and one draw needn't show every extreme that they name: `key_ids`: an event in block o of a device has a key in o * 4096 to (o + 1) * 4096 - 1 that is not a heavy key; every event outside all blocks has a heavy key. `heavy_ids`: distinct keys. `block_offsets`: on each device the blocks lie in the order of o, do not meet, and end by position 8192. `block_counts`: at most 64; one owner gets exactly 64 from every device.
All inputs are finite; a program needn't handle non-finite values.
Results may differ from the reference program's by a relative error of at most 0.000075.
Values sent between devices are 32-bit elements; how exact they have to be, the bound alone decides.
No kernel may reach another device: no remote copies, remote signals or barrier semaphores. Data moves between devices by JAX's collectives and lax.ppermute only.
A program may use at most 64 MiB of HBM per device.

```python
import jax
import jax.numpy as jnp

F = 128
H = 2048
KEYS_DEV = 4096
CAP = 64
EV_DEV = 8192
KEYS = 262144
EVENTS = 1048576
N_REP = 2
N_OWN = 64


def layout_draw(key):
    devices = N_REP * N_OWN
    keys_all = KEYS_DEV * N_OWN
    shuffled = jax.random.permutation(jax.random.fold_in(key, 11), keys_all).astype(jnp.int32)
    heavy = shuffled[:H]
    flags = jnp.zeros((keys_all,), jnp.int32).at[heavy].set(1)
    per_owner = flags.reshape(N_OWN, KEYS_DEV)
    light_order = jnp.argsort(per_owner, axis=1, stable=True).astype(jnp.int32)
    light_count = (KEYS_DEV - jnp.sum(per_owner, axis=1)).astype(jnp.int32)
    lowest = CAP // 8
    owner_top = jax.random.randint(jax.random.fold_in(key, 12), (N_OWN,), CAP // 4, CAP + 1)
    counts = lowest + jax.random.randint(jax.random.fold_in(key, 13), (devices, N_OWN), 0, 1 << 20) % (owner_top - lowest + 1)[None, :]
    target = jax.random.randint(jax.random.fold_in(key, 14), (), 0, N_OWN)
    counts = counts.at[:, target].set(CAP)
    chosen = jax.random.randint(jax.random.fold_in(key, 15), (devices,), 0, N_OWN)
    counts = counts.at[jnp.arange(devices), chosen].set(CAP).astype(jnp.int32)
    spare = EV_DEV - jnp.sum(counts, axis=1)
    gaps = jax.random.randint(jax.random.fold_in(key, 16), (devices, N_OWN), 0, 1 << 20) % (spare[:, None] + 1)
    gaps = jnp.sort(gaps, axis=1)
    offsets = (jnp.cumsum(counts, axis=1) - counts + gaps).astype(jnp.int32)
    positions = jnp.arange(EV_DEV, dtype=jnp.int32)
    member = (positions[None, :, None] >= offsets[:, None, :]) & (positions[None, :, None] < (offsets + counts)[:, None, :])
    in_block = jnp.any(member, axis=2)
    owner = jnp.sum(member.astype(jnp.int32) * jnp.arange(N_OWN, dtype=jnp.int32)[None, None, :], axis=2)
    pick_light = jax.random.randint(jax.random.fold_in(key, 17), (devices, EV_DEV), 0, 1 << 20) % light_count[owner]
    light_key = owner * KEYS_DEV + light_order[owner, pick_light]
    first = jax.random.randint(jax.random.fold_in(key, 18), (devices, EV_DEV), 0, H)
    second = jax.random.randint(jax.random.fold_in(key, 19), (devices, EV_DEV), 0, H)
    third = jax.random.randint(jax.random.fold_in(key, 20), (devices, EV_DEV), 0, H)
    heavy_key = heavy[jnp.minimum(jnp.minimum(first, second), third)]
    key_ids = jnp.where(in_block, light_key, heavy_key).astype(jnp.int32).reshape(-1)
    return (key_ids, heavy, offsets, counts)


def draw_key_ids(key, part):
    return layout_draw(key)[0]


def draw_heavy_ids(key, part):
    return layout_draw(key)[1]


def draw_block_offsets(key, part):
    return layout_draw(key)[2]


def draw_block_counts(key, part):
    return layout_draw(key)[3]


def block_scale(stream_key, dims, cuts, low, high):
    level = 1.0
    for position, parts in cuts:
        steps = jax.random.uniform(jax.random.fold_in(jax.random.fold_in(stream_key, 6), position), (parts,), jnp.float32, low / len(cuts), high / len(cuts))
        level = level * jnp.repeat(jnp.exp(steps), dims[position] // parts).reshape((-1,) + (1,) * (len(dims) - 1 - position))
    return level


def normal_values(own_key, shape, deviation, reach, split=(), kind=jnp.bfloat16):
    factor_of = block_scale(own_key, shape, split, -0.22, 0.18) if split else 1.0
    drawn = jax.random.normal(own_key, shape, jnp.float32) * deviation * factor_of
    return jnp.minimum(jnp.maximum(drawn, -reach), reach).astype(kind)


def setup_inputs(seed: int = 0) -> dict:
    key_list = jax.random.split(jax.random.key(seed), 6)
    return {
        "values": normal_values(key_list[0], (EVENTS, F), 0.1, 0.8, ((0, 128),), jnp.float32),
        "key_ids": draw_key_ids(jax.random.fold_in(key_list[5], 71), 0),
        "heavy_ids": draw_heavy_ids(jax.random.fold_in(key_list[5], 71), 0),
        "block_offsets": draw_block_offsets(jax.random.fold_in(key_list[5], 71), 0),
        "block_counts": draw_block_counts(jax.random.fold_in(key_list[5], 71), 0),
    }


def reference(values, key_ids, heavy_ids, block_offsets, block_counts):
    positions = jnp.arange(EV_DEV, dtype=jnp.int32)
    starts = block_offsets[:, None, :]
    finish = (block_offsets + block_counts)[:, None, :]
    inside = jnp.any((positions[None, :, None] >= starts) & (positions[None, :, None] < finish), axis=2)
    inside = inside.reshape(-1)
    light_keys = jnp.where(inside, key_ids, KEYS).astype(jnp.int32)
    light_sums = jax.ops.segment_sum(values, light_keys, num_segments=KEYS + 1)[:KEYS]
    totals = jax.ops.segment_sum(values, key_ids, num_segments=KEYS)
    heavy_sums = totals[heavy_ids]
    return light_sums, heavy_sums
```

```python
import jax
import jax.numpy as jnp
from jax import lax
from jax.experimental import pallas as pl
from jax.experimental.pallas import tpu as pltpu
from jax.sharding import PartitionSpec as P

KEYS_DEV = 4096
CAP = 64
LANES = 128
BANKS = 8
CHUNK = 32


def pack_blocks(offs, cnts, keys, values, owners, reps):
    events, width = values.shape
    key_rows = events // LANES
    block = CAP + 1

    def body(off_ref, cnt_ref, keys_ref, val_ref, out_ref, buf, krow, arow, sem):
        lane = lax.broadcasted_iota(jnp.int32, (1, LANES), 1)

        def step(o, carry):
            off = off_ref[0, o]
            cnt = cnt_ref[0, o]
            start = jnp.minimum(off, events - CAP)
            row = start // LANES
            shift = start - row * LANES
            row_next = jnp.minimum(row + 1, key_rows - 1)
            first = lane >= shift
            pos = jnp.where(first, row * LANES + lane, (row + 1) * LANES + lane)
            key = jnp.where(first, keys_ref[pl.ds(row, 1), :], keys_ref[pl.ds(row_next, 1), :])
            inside = (pos >= off) & (pos < off + cnt)
            krow[pl.ds(o, 1), :] = jnp.where(inside, key - o * KEYS_DEV, KEYS_DEV)
            arow[pl.ds(o, 1), :] = jnp.full((1, LANES), shift, jnp.int32)
            buf[pl.ds(o * block, CAP), :] = val_ref[pl.ds(start, CAP), :]
            return carry

        lax.fori_loop(0, owners, step, 0, unroll=8)
        rolled = krow[...]
        shifts = arow[...]
        for bit in range(7):
            moved = pltpu.roll(rolled, LANES - (1 << bit), 1)
            rolled = jnp.where((shifts >> bit) & 1 == 1, moved, rolled)
        krow[...] = rolled
        for o in range(owners):
            buf[pl.ds(o * block + CAP, 1), :] = krow[pl.ds(o, 1), :].astype(jnp.float32)
        copies = [pltpu.make_async_copy(buf, out_ref.at[r], sem.at[r]) for r in range(reps)]
        for copy in copies:
            copy.start()
        for copy in copies:
            copy.wait()

    smem = pl.BlockSpec(memory_space=pltpu.SMEM)
    vmem = pl.BlockSpec(memory_space=pltpu.VMEM)
    packed = pl.pallas_call(
        body,
        out_shape=jax.ShapeDtypeStruct((reps, owners * block, width), jnp.float32),
        in_specs=[smem, smem, vmem, vmem],
        out_specs=pl.BlockSpec(memory_space=pl.ANY),
        scratch_shapes=[
            pltpu.VMEM((owners * block, width), jnp.float32),
            pltpu.VMEM((owners, LANES), jnp.int32),
            pltpu.VMEM((owners, LANES), jnp.int32),
            pltpu.SemaphoreType.DMA((reps,)),
        ],
        name="pack_blocks",
    )(offs, cnts, keys.reshape(key_rows, LANES), values)
    return packed.reshape(reps * owners, block, 1, width)


def light_kernel(recv):
    senders, block, _, width = recv.shape
    chunks = senders // CHUNK

    def body(recv_ref, out_ref, rows, kint, ksm, *rest):
        acc = rest[:BANKS]
        key_sem, smem_sem, row_sems = rest[BANKS:]
        key_copy = pltpu.make_async_copy(recv_ref.at[:, CAP], rows.at[:, CAP], key_sem)
        key_copy.start()
        copies = []
        for c in range(chunks):
            part = (pl.ds(c * CHUNK, CHUNK), pl.ds(0, CAP))
            copies.append(
                pltpu.make_async_copy(recv_ref.at[part], rows.at[part], row_sems.at[c])
            )
            copies[c].start()
        key_copy.wait()

        def convert(i, carry):
            kint[i] = rows[i, CAP].astype(jnp.int32)
            return carry

        lax.fori_loop(0, senders, convert, 0, unroll=8)
        smem_copy = pltpu.make_async_copy(kint, ksm, smem_sem)
        smem_copy.start()
        zeros = jnp.zeros((64, width), jnp.float32)

        def clear(i, carry):
            for bank in acc:
                bank[pl.ds(i * 64, 64), :] = zeros
            return carry

        lax.fori_loop(0, KEYS_DEV // 64, clear, 0)
        smem_copy.wait()

        def sender(i, carry):
            for s in range(CAP):
                bank = acc[s % BANKS]
                key = ksm[i, 0, s]
                bank[pl.ds(key, 1), :] = bank[pl.ds(key, 1), :] + rows[i, s]
            return carry

        for c in range(chunks):
            copies[c].wait()
            lax.fori_loop(c * CHUNK, (c + 1) * CHUNK, sender, 0)

        def finish(i, carry):
            span = pl.ds(i * 64, 64)
            total = acc[0][span, :]
            for bank in acc[1:]:
                total = total + bank[span, :]
            out_ref[span, :] = total
            return carry

        lax.fori_loop(0, KEYS_DEV // 64, finish, 0)

    return pl.pallas_call(
        body,
        out_shape=jax.ShapeDtypeStruct((KEYS_DEV, width), jnp.float32),
        in_specs=[pl.BlockSpec(memory_space=pl.ANY)],
        out_specs=pl.BlockSpec(memory_space=pltpu.VMEM),
        scratch_shapes=[
            pltpu.VMEM((senders, block, 1, width), jnp.float32),
            pltpu.VMEM((senders, 1, width), jnp.int32),
            pltpu.SMEM((senders, 1, width), jnp.int32),
        ]
        + [pltpu.VMEM((KEYS_DEV + 8, width), jnp.float32) for _ in range(BANKS)]
        + [
            pltpu.SemaphoreType.DMA,
            pltpu.SemaphoreType.DMA,
            pltpu.SemaphoreType.DMA((chunks,)),
        ],
        name="light_sums",
    )(recv)


def heavy_kernel(values, keys, heavy_ids):
    events, width = values.shape
    heavy = heavy_ids.shape[0]
    step_events = 2048
    tile = 512
    rows = step_events // LANES
    steps = events // step_events

    def body(h_ref, k_ref, v_ref, out_ref, ids, acc):
        c = pl.program_id(0)

        @pl.when(c == 0)
        def _():
            ids[...] = jnp.broadcast_to(h_ref[...], ids.shape)

        v = v_ref[...]
        high = v.astype(jnp.bfloat16)
        low = (v - high.astype(jnp.float32)).astype(jnp.bfloat16)
        rhs = jnp.concatenate([high, low], axis=1)
        key_rows = [k_ref[pl.ds(c * rows + j, 1), :] for j in range(rows)]
        for t in range(heavy // tile):
            span = pl.ds(t * tile, tile)
            h = ids[span, :]
            onehot = jnp.concatenate(
                [jnp.where(h == row, 1.0, 0.0).astype(jnp.bfloat16) for row in key_rows], axis=1
            )
            added = jnp.dot(onehot, rhs, preferred_element_type=jnp.float32)

            @pl.when(c == 0)
            def _():
                acc[span, :] = added

            @pl.when(c != 0)
            def _():
                acc[span, :] += added

        @pl.when(c == steps - 1)
        def _():
            out_ref[...] = acc[:, :width] + acc[:, width:]

    return pl.pallas_call(
        body,
        grid=(steps,),
        out_shape=jax.ShapeDtypeStruct((heavy, width), jnp.float32),
        in_specs=[
            pl.BlockSpec((heavy, 1), lambda c: (0, 0)),
            pl.BlockSpec((events // LANES, LANES), lambda c: (0, 0)),
            pl.BlockSpec((step_events, width), lambda c: (c, 0)),
        ],
        out_specs=pl.BlockSpec((heavy, width), lambda c: (0, 0)),
        scratch_shapes=[
            pltpu.VMEM((heavy, LANES), jnp.int32),
            pltpu.VMEM((heavy, 2 * width), jnp.float32),
        ],
        cost_estimate=pl.CostEstimate(
            flops=4 * events * heavy * width, bytes_accessed=4 * events * width, transcendentals=0
        ),
        name="heavy_sums",
    )(heavy_ids.reshape(heavy, 1), keys.reshape(events // LANES, LANES), values)


def per_device(values, key_ids, heavy_ids, block_offsets, block_counts):
    owners = lax.axis_size("own")
    pairs = lax.axis_size("rep")
    packed = pack_blocks(block_offsets, block_counts, key_ids, values, owners, pairs)
    recv = lax.all_to_all(packed, ("rep", "own"), split_axis=0, concat_axis=0, tiled=True)
    partial = heavy_kernel(values, key_ids, heavy_ids)
    heavy, width = partial.shape
    pieces = lax.all_to_all(
        partial.reshape(owners, heavy // owners, width), "own", 0, 0, tiled=True
    )
    mine = jnp.sum(pieces, axis=0)
    heavy_sums = mine + lax.ppermute(mine, "rep", [(0, 1), (1, 0)])
    light_sums = light_kernel(recv)
    return (light_sums, heavy_sums)


def solution(mesh):
    placed = (
        P(("rep", "own"), None),
        P(("rep", "own")),
        P(),
        P(("rep", "own"), None),
        P(("rep", "own"), None),
    )
    return jax.shard_map(
        per_device,
        mesh=mesh,
        in_specs=placed,
        out_specs=(P("own", None), P("own", None)),
        check_vma=False,
    )
```

```python
import jax
import jax.numpy as jnp
from jax import lax
from jax.experimental import pallas as pl
from jax.experimental.pallas import tpu as pltpu
from jax.sharding import PartitionSpec as P

KEYS_DEV = 4096
CAP = 64
LANES = 128
BANKS = 8
CHUNK = 32


def pack_blocks(offs, cnts, keys, values, owners, reps):
    events, width = values.shape
    key_rows = events // LANES
    block = CAP + 1

    def body(off_ref, cnt_ref, keys_ref, val_ref, out_ref, buf, krow, arow, sem):
        lane = lax.broadcasted_iota(jnp.int32, (1, LANES), 1)

        def step(o, carry):
            off = off_ref[0, o]
            cnt = cnt_ref[0, o]
            start = jnp.minimum(off, events - CAP)
            row = start // LANES
            shift = start - row * LANES
            row_next = jnp.minimum(row + 1, key_rows - 1)
            first = lane >= shift
            pos = jnp.where(first, row * LANES + lane, (row + 1) * LANES + lane)
            key = jnp.where(first, keys_ref[pl.ds(row, 1), :], keys_ref[pl.ds(row_next, 1), :])
            inside = (pos >= off) & (pos < off + cnt)
            krow[pl.ds(o, 1), :] = jnp.where(inside, key - o * KEYS_DEV, KEYS_DEV)
            arow[pl.ds(o, 1), :] = jnp.full((1, LANES), shift, jnp.int32)
            buf[pl.ds(o * block, CAP), :] = val_ref[pl.ds(start, CAP), :]
            return carry

        lax.fori_loop(0, owners, step, 0, unroll=8)
        rolled = krow[...]
        shifts = arow[...]
        for bit in range(7):
            moved = pltpu.roll(rolled, LANES - (1 << bit), 1)
            rolled = jnp.where((shifts >> bit) & 1 == 1, moved, rolled)
        krow[...] = rolled
        for o in range(owners):
            buf[pl.ds(o * block + CAP, 1), :] = krow[pl.ds(o, 1), :].astype(jnp.float32)
        copies = [pltpu.make_async_copy(buf, out_ref.at[r], sem.at[r]) for r in range(reps)]
        for copy in copies:
            copy.start()
        for copy in copies:
            copy.wait()

    smem = pl.BlockSpec(memory_space=pltpu.SMEM)
    vmem = pl.BlockSpec(memory_space=pltpu.VMEM)
    packed = pl.pallas_call(
        body,
        out_shape=jax.ShapeDtypeStruct((reps, owners * block, width), jnp.float32),
        in_specs=[smem, smem, vmem, vmem],
        out_specs=pl.BlockSpec(memory_space=pl.ANY),
        scratch_shapes=[
            pltpu.VMEM((owners * block, width), jnp.float32),
            pltpu.VMEM((owners, LANES), jnp.int32),
            pltpu.VMEM((owners, LANES), jnp.int32),
            pltpu.SemaphoreType.DMA((reps,)),
        ],
        name="pack_blocks",
    )(offs, cnts, keys.reshape(key_rows, LANES), values)
    return packed.reshape(reps * owners, block, 1, width)


def light_kernel(recv):
    senders, block, _, width = recv.shape
    chunks = senders // CHUNK

    def body(recv_ref, out_ref, rows, kint, ksm, *rest):
        acc = rest[:BANKS]
        key_sem, smem_sem, row_sems = rest[BANKS:]
        key_copy = pltpu.make_async_copy(recv_ref.at[:, CAP], rows.at[:, CAP], key_sem)
        key_copy.start()
        copies = []
        for c in range(chunks):
            part = (pl.ds(c * CHUNK, CHUNK), pl.ds(0, CAP))
            copies.append(
                pltpu.make_async_copy(recv_ref.at[part], rows.at[part], row_sems.at[c])
            )
            copies[c].start()
        key_copy.wait()

        def convert(i, carry):
            kint[i] = rows[i, CAP].astype(jnp.int32)
            return carry

        lax.fori_loop(0, senders, convert, 0, unroll=8)
        smem_copy = pltpu.make_async_copy(kint, ksm, smem_sem)
        smem_copy.start()
        zeros = jnp.zeros((64, width), jnp.float32)

        def clear(i, carry):
            for bank in acc:
                bank[pl.ds(i * 64, 64), :] = zeros
            return carry

        lax.fori_loop(0, KEYS_DEV // 64, clear, 0)
        smem_copy.wait()

        def sender(i, carry):
            for s in range(CAP):
                bank = acc[s % BANKS]
                key = ksm[i, 0, s]
                bank[pl.ds(key, 1), :] = bank[pl.ds(key, 1), :] + rows[i, s]
            return carry

        for c in range(chunks):
            copies[c].wait()
            lax.fori_loop(c * CHUNK, (c + 1) * CHUNK, sender, 0)

        def finish(i, carry):
            span = pl.ds(i * 64, 64)
            total = acc[0][span, :]
            for bank in acc[1:]:
                total = total + bank[span, :]
            out_ref[span, :] = total
            return carry

        lax.fori_loop(0, KEYS_DEV // 64, finish, 0)

    return pl.pallas_call(
        body,
        out_shape=jax.ShapeDtypeStruct((KEYS_DEV, width), jnp.float32),
        in_specs=[pl.BlockSpec(memory_space=pl.ANY)],
        out_specs=pl.BlockSpec(memory_space=pltpu.VMEM),
        scratch_shapes=[
            pltpu.VMEM((senders, block, 1, width), jnp.float32),
            pltpu.VMEM((senders, 1, width), jnp.int32),
            pltpu.SMEM((senders, 1, width), jnp.int32),
        ]
        + [pltpu.VMEM((KEYS_DEV + 8, width), jnp.float32) for _ in range(BANKS)]
        + [
            pltpu.SemaphoreType.DMA,
            pltpu.SemaphoreType.DMA,
            pltpu.SemaphoreType.DMA((chunks,)),
        ],
        name="light_sums",
    )(recv)


def heavy_kernel(values, keys, heavy_ids, place):
    events, width = values.shape
    heavy = heavy_ids.shape[0]
    tile = heavy // 2
    step_events = 2048
    event_rows = events // LANES
    rows = step_events // LANES
    nx, nz, ny, nc = 4, 4, 2, 2
    piece = heavy // (nx * nz * ny * nc)

    def body(at_ref, h_ref, k_ref, v_ref, near_ref, far_ref, ids, rhs):
        c = pl.program_id(0)

        @pl.when(c == 0)
        def _():
            for p in range(nx * nz * ny * nc):
                dc, dx, dz, dy = p // 32, (p // 8) % 4, (p // 2) % 4, p % 2
                x = (at_ref[0] + dx) % nx
                z = (at_ref[1] + dz) % nz
                y = (at_ref[2] + dy) % ny
                core = (at_ref[3] + dc) % nc
                source = ((x * nz + z) * ny + y) * nc + core
                column = h_ref[pl.ds(pl.multiple_of(source * piece, piece), piece), :]
                ids[pl.ds(p * piece, piece), :] = jnp.broadcast_to(column, (piece, LANES))

            def split(i, carry):
                span = pl.ds(i * 512, 512)
                v = v_ref[span, :]
                high = v.astype(jnp.bfloat16)
                rhs[span, :width] = high
                rhs[span, width:] = (v - high.astype(jnp.float32)).astype(jnp.bfloat16)
                return carry

            lax.fori_loop(0, events // 512, split, 0)

        h = ids[pl.ds(c * tile, tile), :]
        total = None
        for q in range(events // step_events):
            onehot = jnp.concatenate(
                [
                    jnp.where(h == k_ref[pl.ds(q * rows + j, 1), :], 1.0, 0.0).astype(jnp.bfloat16)
                    for j in range(rows)
                ],
                axis=1,
            )
            added = jnp.dot(
                onehot,
                rhs[pl.ds(q * step_events, step_events), :],
                preferred_element_type=jnp.float32,
            )
            total = added if total is None else total + added

        @pl.when(c == 0)
        def _():
            near_ref[...] = total[:, :width] + total[:, width:]

        @pl.when(c == 1)
        def _():
            far_ref[...] = total[:, :width] + total[:, width:]

    half = jax.ShapeDtypeStruct((tile, width), jnp.float32)
    return pl.pallas_call(
        body,
        grid=(2,),
        out_shape=(half, half),
        in_specs=[
            pl.BlockSpec(memory_space=pltpu.SMEM),
            pl.BlockSpec((heavy, 1), lambda c: (0, 0)),
            pl.BlockSpec((event_rows, LANES), lambda c: (0, 0)),
            pl.BlockSpec((events, width), lambda c: (0, 0)),
        ],
        out_specs=(
            pl.BlockSpec((tile, width), lambda c: (0, 0)),
            pl.BlockSpec((tile, width), lambda c: (0, 0)),
        ),
        scratch_shapes=[
            pltpu.VMEM((heavy, LANES), jnp.int32),
            pltpu.VMEM((events, 2 * width), jnp.bfloat16),
        ],
        name="heavy_sums",
    )(place, heavy_ids.reshape(heavy, 1), keys.reshape(event_rows, LANES), values)


def ring_sum(x, axis):
    size = x.shape[0]
    total = x[0]
    for d in range(1, size):
        total = total + lax.ppermute(x[d], axis, [(i, (i + d) % size) for i in range(size)])
    return total


def per_device(values, key_ids, heavy_ids, block_offsets, block_counts):
    own = ("x", "z", "y_hi", "core")
    owners = lax.axis_size(own)
    pairs = lax.axis_size("rep")
    place = jnp.stack([lax.axis_index(axis) for axis in own]).astype(jnp.int32)
    packed = pack_blocks(block_offsets, block_counts, key_ids, values, owners, pairs)
    recv = lax.all_to_all(packed, ("rep",) + own, split_axis=0, concat_axis=0, tiled=True)
    near, far = heavy_kernel(values, key_ids, heavy_ids, place)
    width = near.shape[1]
    near = near + lax.ppermute(far, "core", [(0, 1), (1, 0)])
    near = ring_sum(near.reshape(4, -1, width), "x")
    near = ring_sum(near.reshape(4, -1, width), "z")
    keep, give = jnp.split(near, 2, axis=0)
    column = ("rep", "y_hi")
    near_rep = keep + lax.ppermute(give, column, [(0, 1), (1, 0), (2, 3), (3, 2)])
    other_rep = lax.ppermute(keep, column, [(0, 2), (2, 0), (1, 3), (3, 1)])
    other_rep = other_rep + lax.ppermute(give, column, [(0, 3), (3, 0), (1, 2), (2, 1)])
    heavy_sums = near_rep + other_rep
    light_sums = light_kernel(recv)
    return (light_sums, heavy_sums)


def solution(mesh):
    own = ("x", "z", "y_hi", "core")
    every = ("rep",) + own
    mesh = jax.sharding.Mesh(mesh.devices.reshape(2, 4, 4, 2, 2), every)
    placed = (P(every, None), P(every), P(), P(every, None), P(every, None))
    return jax.shard_map(
        per_device,
        mesh=mesh,
        in_specs=placed,
        out_specs=(P(own, None), P(own, None)),
        check_vma=False,
    )
```

```python
import jax
import jax.numpy as jnp
from jax import lax
from jax.experimental import pallas as pl
from jax.experimental.pallas import tpu as pltpu
from jax.sharding import PartitionSpec as P

KEYS_DEV = 4096
CAP = 64
LANES = 128
BANKS = 8
CHUNK = 32


def pack_blocks(offs, cnts, keys, values, sizes):
    nr, nx, nz, ny, nc = sizes
    events, width = values.shape
    key_rows = events // LANES
    block = CAP + 1
    groups, members = nz * ny, nx * nc
    owners = groups * members

    def owner_of(g, m):
        return (((m // nc) * nz + g // ny) * ny + g % ny) * nc + m % nc

    def body(off_ref, cnt_ref, keys_ref, val_ref, out_ref, rows, buf, krow, arow, in_sem, out_sem):
        lane = lax.broadcasted_iota(jnp.int32, (1, LANES), 1)

        load = pltpu.make_async_copy(val_ref, rows, in_sem)
        load.start()

        def block_keys(b, carry):
            o = owner_of(b // members, b % members)
            off = off_ref[0, o]
            end = off + cnt_ref[0, o]
            start = jnp.minimum(off, events - CAP)
            row = start // LANES
            shift = start - row * LANES
            row_next = jnp.minimum(row + 1, key_rows - 1)
            first = lane >= shift
            pos = jnp.where(first, row * LANES + lane, (row + 1) * LANES + lane)
            key = jnp.where(first, keys_ref[pl.ds(row, 1), :], keys_ref[pl.ds(row_next, 1), :])
            inside = (pos >= off) & (pos < end)
            krow[pl.ds(b, 1), :] = jnp.where(inside, key - o * KEYS_DEV, KEYS_DEV)
            arow[pl.ds(b, 1), :] = jnp.full((1, LANES), shift, jnp.int32)
            return carry

        lax.fori_loop(0, owners, block_keys, 0, unroll=16)
        rolled = krow[...]
        shifts = arow[...]
        for bit in range(7):
            moved = pltpu.roll(rolled, LANES - (1 << bit), 1)
            rolled = jnp.where((shifts >> bit) & 1 == 1, moved, rolled)
        krow[...] = rolled
        load.wait()
        stores = []
        for g in range(groups):
            for m in range(members):
                b = g * members + m
                start = jnp.minimum(off_ref[0, owner_of(g, m)], events - CAP)
                buf[pl.ds(b * block, CAP), :] = rows[pl.ds(start, CAP), :]
                buf[pl.ds(b * block + CAP, 1), :] = krow[pl.ds(b, 1), :].astype(jnp.float32)
            span = pl.ds(g * members * block, members * block)
            for r in range(nr):
                store = pltpu.make_async_copy(
                    buf.at[span], out_ref.at[g * nr + r], out_sem.at[g * nr + r]
                )
                store.start()
                stores.append(store)
        for store in stores:
            store.wait()

    smem = pl.BlockSpec(memory_space=pltpu.SMEM)
    packed = pl.pallas_call(
        body,
        out_shape=jax.ShapeDtypeStruct((groups * nr, members * block, width), jnp.float32),
        in_specs=[
            smem,
            smem,
            pl.BlockSpec(memory_space=pltpu.VMEM),
            pl.BlockSpec(memory_space=pl.ANY),
        ],
        out_specs=pl.BlockSpec(memory_space=pl.ANY),
        scratch_shapes=[
            pltpu.VMEM((events, width), jnp.float32),
            pltpu.VMEM((owners * block, width), jnp.float32),
            pltpu.VMEM((owners, LANES), jnp.int32),
            pltpu.VMEM((owners, LANES), jnp.int32),
            pltpu.SemaphoreType.DMA,
            pltpu.SemaphoreType.DMA((groups * nr,)),
        ],
        name="pack_blocks",
    )(offs, cnts, keys.reshape(key_rows, LANES), values)
    return packed.reshape(nr * owners, block, 1, width)


def light_kernel(recv):
    senders, block, _, width = recv.shape
    chunks = senders // CHUNK

    def body(recv_ref, out_ref, rows, kint, ksm, *rest):
        acc = rest[:BANKS]
        key_sem, smem_sem, row_sems, out_sems = rest[BANKS:]
        key_copy = pltpu.make_async_copy(recv_ref.at[:, CAP], rows.at[:, CAP], key_sem)
        key_copy.start()
        copies = []
        for c in range(chunks):
            part = (pl.ds(c * CHUNK, CHUNK), pl.ds(0, CAP))
            copies.append(
                pltpu.make_async_copy(recv_ref.at[part], rows.at[part], row_sems.at[c])
            )
            copies[c].start()
        key_copy.wait()

        def convert(i, carry):
            kint[i] = rows[i, CAP].astype(jnp.int32)
            return carry

        lax.fori_loop(0, senders, convert, 0, unroll=8)
        smem_copy = pltpu.make_async_copy(kint, ksm, smem_sem)
        smem_copy.start()
        zeros = jnp.zeros((64, width), jnp.float32)

        def clear(i, carry):
            for bank in acc:
                bank[pl.ds(i * 64, 64), :] = zeros
            return carry

        lax.fori_loop(0, KEYS_DEV // 64, clear, 0)
        smem_copy.wait()

        def sender(i, carry):
            for s in range(CAP):
                bank = acc[s % BANKS]
                key = ksm[i, 0, s]
                bank[pl.ds(key, 1), :] = bank[pl.ds(key, 1), :] + rows[i, s]
            return carry

        for c in range(chunks):
            copies[c].wait()
            lax.fori_loop(c * CHUNK, (c + 1) * CHUNK, sender, 0)

        def finish(i, carry):
            span = pl.ds(i * 64, 64)
            total = acc[0][span, :]
            for bank in acc[1:]:
                total = total + bank[span, :]
            acc[0][span, :] = total
            return carry

        parts = 8
        stores = []
        for c in range(parts):
            step = KEYS_DEV // parts
            lax.fori_loop(c * step // 64, (c + 1) * step // 64, finish, 0)
            span = pl.ds(c * step, step)
            stores.append(pltpu.make_async_copy(acc[0].at[span], out_ref.at[span], out_sems.at[c]))
            stores[c].start()
        for store in stores:
            store.wait()

    return pl.pallas_call(
        body,
        out_shape=jax.ShapeDtypeStruct((KEYS_DEV, width), jnp.float32),
        in_specs=[pl.BlockSpec(memory_space=pl.ANY)],
        out_specs=pl.BlockSpec(memory_space=pl.ANY),
        scratch_shapes=[
            pltpu.VMEM((senders, block, 1, width), jnp.float32),
            pltpu.VMEM((senders, 1, width), jnp.int32),
            pltpu.SMEM((senders, 1, width), jnp.int32),
        ]
        + [pltpu.VMEM((KEYS_DEV + 8, width), jnp.float32) for _ in range(BANKS)]
        + [
            pltpu.SemaphoreType.DMA,
            pltpu.SemaphoreType.DMA,
            pltpu.SemaphoreType.DMA((chunks,)),
            pltpu.SemaphoreType.DMA((8,)),
        ],
        name="light_sums",
    )(recv)


def heavy_kernel(values, keys, heavy_ids, core, owners):
    events, width = values.shape
    heavy = heavy_ids.shape[0]
    tile = heavy // 2
    step_events = 2048
    event_rows = events // LANES
    rows = step_events // LANES
    half = owners // 2
    piece = heavy // owners

    def body(core_ref, h_ref, k_ref, v_ref, near_ref, far_ref, ids, rhs):
        c = pl.program_id(0)

        @pl.when(c == 0)
        def _():
            for p in range(owners):
                source = (p % half) * 2 + (core_ref[0] + p // half) % 2
                column = h_ref[pl.ds(pl.multiple_of(source * piece, piece), piece), :]
                ids[pl.ds(p * piece, piece), :] = jnp.broadcast_to(column, (piece, LANES))

            def split(i, carry):
                span = pl.ds(i * 512, 512)
                v = v_ref[span, :]
                high = v.astype(jnp.bfloat16)
                rhs[span, :width] = high
                rhs[span, width:] = (v - high.astype(jnp.float32)).astype(jnp.bfloat16)
                return carry

            lax.fori_loop(0, events // 512, split, 0)

        h = ids[pl.ds(c * tile, tile), :]
        total = None
        for q in range(events // step_events):
            onehot = jnp.concatenate(
                [
                    jnp.where(h == k_ref[pl.ds(q * rows + j, 1), :], 1.0, 0.0).astype(jnp.bfloat16)
                    for j in range(rows)
                ],
                axis=1,
            )
            added = jnp.dot(
                onehot,
                rhs[pl.ds(q * step_events, step_events), :],
                preferred_element_type=jnp.float32,
            )
            total = added if total is None else total + added

        @pl.when(c == 0)
        def _():
            near_ref[...] = total[:, :width] + total[:, width:]

        @pl.when(c == 1)
        def _():
            far_ref[...] = total[:, :width] + total[:, width:]

    side = jax.ShapeDtypeStruct((tile, width), jnp.float32)
    return pl.pallas_call(
        body,
        grid=(2,),
        out_shape=(side, side),
        in_specs=[
            pl.BlockSpec(memory_space=pltpu.SMEM),
            pl.BlockSpec((heavy, 1), lambda c: (0, 0)),
            pl.BlockSpec((event_rows, LANES), lambda c: (0, 0)),
            pl.BlockSpec((events, width), lambda c: (0, 0)),
        ],
        out_specs=(
            pl.BlockSpec((tile, width), lambda c: (0, 0)),
            pl.BlockSpec((tile, width), lambda c: (0, 0)),
        ),
        scratch_shapes=[
            pltpu.VMEM((heavy, LANES), jnp.int32),
            pltpu.VMEM((events, 2 * width), jnp.bfloat16),
        ],
        name="heavy_sums",
    )(core, heavy_ids.reshape(heavy, 1), keys.reshape(event_rows, LANES), values)


def per_device(values, key_ids, heavy_ids, block_offsets, block_counts):
    own = ("x", "z", "y_hi", "core")
    sizes = tuple(lax.axis_size(axis) for axis in ("rep",) + own)
    owners = lax.axis_size(own)
    packed = pack_blocks(block_offsets, block_counts, key_ids, values, sizes)
    order = ("z", "y_hi", "rep", "x", "core")
    recv = lax.all_to_all(packed, order, split_axis=0, concat_axis=0, tiled=True)
    core = lax.axis_index("core").astype(jnp.int32).reshape(1)
    near, far = heavy_kernel(values, key_ids, heavy_ids, core, owners)
    near = near + lax.ppermute(far, "core", [(0, 1), (1, 0)])
    pieces = near.reshape(owners // 2, -1, near.shape[1])
    pieces = jnp.concatenate([pieces, pieces], axis=0)
    pieces = lax.all_to_all(pieces, ("rep", "x", "z", "y_hi"), 0, 0, tiled=True)
    light_sums = light_kernel(recv)
    heavy_sums = jnp.sum(pieces, axis=0)
    return (light_sums, heavy_sums)


def solution(mesh):
    own = ("x", "z", "y_hi", "core")
    every = ("rep",) + own
    mesh = jax.sharding.Mesh(mesh.devices.reshape(2, 4, 4, 2, 2), every)
    placed = (P(every, None), P(every), P(), P(every, None), P(every, None))
    return jax.shard_map(
        per_device,
        mesh=mesh,
        in_specs=placed,
        out_specs=(P(own, None), P(own, None)),
        check_vma=False,
    )
```

```python
import jax
import jax.numpy as jnp
from jax import lax
from jax.experimental import pallas as pl
from jax.experimental.pallas import tpu as pltpu
from jax.sharding import PartitionSpec as P

KEYS_DEV = 4096
CAP = 64
LANES = 128
BANKS = 8
CHUNK = 32


def pack_blocks(offs, cnts, keys, values, sizes):
    nr, nx, nz, ny, nc = sizes
    events, width = values.shape
    key_rows = events // LANES
    block = CAP + 1
    groups, members = nz * ny, nx * nc
    owners = groups * members

    def owner_of(g, m):
        return (((m // nc) * nz + g // ny) * ny + g % ny) * nc + m % nc

    def body(off_ref, cnt_ref, keys_ref, val_ref, out_ref, rows, buf, krow, arow, in_sem, out_sem):
        lane = lax.broadcasted_iota(jnp.int32, (1, LANES), 1)

        load = pltpu.make_async_copy(val_ref, rows, in_sem)
        load.start()

        def block_keys(b, carry):
            o = owner_of(b // members, b % members)
            off = off_ref[0, o]
            end = off + cnt_ref[0, o]
            start = jnp.minimum(off, events - CAP)
            row = start // LANES
            shift = start - row * LANES
            row_next = jnp.minimum(row + 1, key_rows - 1)
            first = lane >= shift
            pos = jnp.where(first, row * LANES + lane, (row + 1) * LANES + lane)
            key = jnp.where(first, keys_ref[pl.ds(row, 1), :], keys_ref[pl.ds(row_next, 1), :])
            inside = (pos >= off) & (pos < end)
            krow[pl.ds(b, 1), :] = jnp.where(inside, key - o * KEYS_DEV, KEYS_DEV)
            arow[pl.ds(b, 1), :] = jnp.full((1, LANES), shift, jnp.int32)
            return carry

        lax.fori_loop(0, owners, block_keys, 0, unroll=16)
        rolled = krow[...]
        shifts = arow[...]
        for bit in range(7):
            moved = pltpu.roll(rolled, LANES - (1 << bit), 1)
            rolled = jnp.where((shifts >> bit) & 1 == 1, moved, rolled)
        krow[...] = rolled
        load.wait()
        stores = []
        for g in range(groups):
            for m in range(members):
                b = g * members + m
                start = jnp.minimum(off_ref[0, owner_of(g, m)], events - CAP)
                buf[pl.ds(b * block, CAP), :] = rows[pl.ds(start, CAP), :]
                buf[pl.ds(b * block + CAP, 1), :] = krow[pl.ds(b, 1), :].astype(jnp.float32)
            span = pl.ds(g * members * block, members * block)
            for r in range(nr):
                store = pltpu.make_async_copy(
                    buf.at[span], out_ref.at[g * nr + r], out_sem.at[g * nr + r]
                )
                store.start()
                stores.append(store)
        for store in stores:
            store.wait()

    smem = pl.BlockSpec(memory_space=pltpu.SMEM)
    packed = pl.pallas_call(
        body,
        out_shape=jax.ShapeDtypeStruct((groups * nr, members * block, width), jnp.float32),
        in_specs=[
            smem,
            smem,
            pl.BlockSpec(memory_space=pltpu.VMEM),
            pl.BlockSpec(memory_space=pl.ANY),
        ],
        out_specs=pl.BlockSpec(memory_space=pl.ANY),
        scratch_shapes=[
            pltpu.VMEM((events, width), jnp.float32),
            pltpu.VMEM((owners * block, width), jnp.float32),
            pltpu.VMEM((owners, LANES), jnp.int32),
            pltpu.VMEM((owners, LANES), jnp.int32),
            pltpu.SemaphoreType.DMA,
            pltpu.SemaphoreType.DMA((groups * nr,)),
        ],
        name="pack_blocks",
    )(offs, cnts, keys.reshape(key_rows, LANES), values)
    return packed.reshape(nr * owners, block, 1, width)


def light_kernel(recv):
    senders, block, _, width = recv.shape
    chunks = senders // CHUNK

    def body(recv_ref, out_ref, rows, kint, ksm, *rest):
        acc = rest[:BANKS]
        key_sem, smem_sem, row_sems, out_sems = rest[BANKS:]
        key_copy = pltpu.make_async_copy(recv_ref.at[:, CAP], rows.at[:, CAP], key_sem)
        key_copy.start()
        copies = []
        for c in range(chunks):
            part = (pl.ds(c * CHUNK, CHUNK), pl.ds(0, CAP))
            copies.append(
                pltpu.make_async_copy(recv_ref.at[part], rows.at[part], row_sems.at[c])
            )
            copies[c].start()
        key_copy.wait()

        def convert(i, carry):
            kint[i] = rows[i, CAP].astype(jnp.int32)
            return carry

        lax.fori_loop(0, senders, convert, 0, unroll=8)
        smem_copy = pltpu.make_async_copy(kint, ksm, smem_sem)
        smem_copy.start()
        zeros = jnp.zeros((64, width), jnp.float32)

        def clear(i, carry):
            for bank in acc:
                bank[pl.ds(i * 64, 64), :] = zeros
            return carry

        lax.fori_loop(0, KEYS_DEV // 64, clear, 0)
        smem_copy.wait()

        def sender(i, carry):
            for s in range(CAP):
                bank = acc[s % BANKS]
                key = ksm[i, 0, s]
                bank[pl.ds(key, 1), :] = bank[pl.ds(key, 1), :] + rows[i, s]
            return carry

        for c in range(chunks):
            copies[c].wait()
            lax.fori_loop(c * CHUNK, (c + 1) * CHUNK, sender, 0)

        def finish(i, carry):
            span = pl.ds(i * 64, 64)
            total = acc[0][span, :]
            for bank in acc[1:]:
                total = total + bank[span, :]
            acc[0][span, :] = total
            return carry

        parts = 8
        stores = []
        for c in range(parts):
            step = KEYS_DEV // parts
            lax.fori_loop(c * step // 64, (c + 1) * step // 64, finish, 0)
            span = pl.ds(c * step, step)
            stores.append(pltpu.make_async_copy(acc[0].at[span], out_ref.at[span], out_sems.at[c]))
            stores[c].start()
        for store in stores:
            store.wait()

    return pl.pallas_call(
        body,
        out_shape=jax.ShapeDtypeStruct((KEYS_DEV, width), jnp.float32),
        in_specs=[pl.BlockSpec(memory_space=pl.ANY)],
        out_specs=pl.BlockSpec(memory_space=pl.ANY),
        scratch_shapes=[
            pltpu.VMEM((senders, block, 1, width), jnp.float32),
            pltpu.VMEM((senders, 1, width), jnp.int32),
            pltpu.SMEM((senders, 1, width), jnp.int32),
        ]
        + [pltpu.VMEM((KEYS_DEV + 8, width), jnp.float32) for _ in range(BANKS)]
        + [
            pltpu.SemaphoreType.DMA,
            pltpu.SemaphoreType.DMA,
            pltpu.SemaphoreType.DMA((chunks,)),
            pltpu.SemaphoreType.DMA((8,)),
        ],
        name="light_sums",
    )(recv)


def heavy_kernel(values, keys, heavy_ids, place, owners, across):
    events, width = values.shape
    heavy = heavy_ids.shape[0]
    tile = heavy // 2
    step_events = 2048
    event_rows = events // LANES
    rows = step_events // LANES
    half = owners // 2
    stride = half // across
    piece = heavy // owners

    def body(at_ref, h_ref, k_ref, v_ref, near_ref, far_ref, ids, rhs):
        c = pl.program_id(0)

        @pl.when(c == 0)
        def _():
            for p in range(owners):
                x = (at_ref[0] + p % half // stride) % (half // stride)
                core = (at_ref[1] + p // half) % 2
                source = (x * stride + p % stride) * 2 + core
                column = h_ref[pl.ds(pl.multiple_of(source * piece, piece), piece), :]
                ids[pl.ds(p * piece, piece), :] = jnp.broadcast_to(column, (piece, LANES))

            def split(i, carry):
                span = pl.ds(i * 512, 512)
                v = v_ref[span, :]
                high = v.astype(jnp.bfloat16)
                rhs[span, :width] = high
                rhs[span, width:] = (v - high.astype(jnp.float32)).astype(jnp.bfloat16)
                return carry

            lax.fori_loop(0, events // 512, split, 0)

        h = ids[pl.ds(c * tile, tile), :]
        total = None
        for q in range(events // step_events):
            onehot = jnp.concatenate(
                [
                    jnp.where(h == k_ref[pl.ds(q * rows + j, 1), :], 1.0, 0.0).astype(jnp.bfloat16)
                    for j in range(rows)
                ],
                axis=1,
            )
            added = jnp.dot(
                onehot,
                rhs[pl.ds(q * step_events, step_events), :],
                preferred_element_type=jnp.float32,
            )
            total = added if total is None else total + added

        @pl.when(c == 0)
        def _():
            near_ref[...] = total[:, :width] + total[:, width:]

        @pl.when(c == 1)
        def _():
            far_ref[...] = total[:, :width] + total[:, width:]

    side = jax.ShapeDtypeStruct((tile, width), jnp.float32)
    return pl.pallas_call(
        body,
        grid=(2,),
        out_shape=(side, side),
        in_specs=[
            pl.BlockSpec(memory_space=pltpu.SMEM),
            pl.BlockSpec((heavy, 1), lambda c: (0, 0)),
            pl.BlockSpec((event_rows, LANES), lambda c: (0, 0)),
            pl.BlockSpec((events, width), lambda c: (0, 0)),
        ],
        out_specs=(
            pl.BlockSpec((tile, width), lambda c: (0, 0)),
            pl.BlockSpec((tile, width), lambda c: (0, 0)),
        ),
        scratch_shapes=[
            pltpu.VMEM((heavy, LANES), jnp.int32),
            pltpu.VMEM((events, 2 * width), jnp.bfloat16),
        ],
        name="heavy_sums",
    )(place, heavy_ids.reshape(heavy, 1), keys.reshape(event_rows, LANES), values)


def per_device(values, key_ids, heavy_ids, block_offsets, block_counts):
    own = ("x", "z", "y_hi", "core")
    sizes = tuple(lax.axis_size(axis) for axis in ("rep",) + own)
    owners = lax.axis_size(own)
    packed = pack_blocks(block_offsets, block_counts, key_ids, values, sizes)
    order = ("z", "y_hi", "rep", "x", "core")
    recv = lax.all_to_all(packed, order, split_axis=0, concat_axis=0, tiled=True)
    across = lax.axis_size("x")
    place = jnp.stack([lax.axis_index("x"), lax.axis_index("core")]).astype(jnp.int32)
    near, far = heavy_kernel(values, key_ids, heavy_ids, place, owners, across)
    width = near.shape[1]
    near = near + lax.ppermute(far, "core", [(0, 1), (1, 0)])
    parts = near.reshape(across, -1, width)
    near = parts[0]
    for d in range(1, across):
        ring = [(i, (i + d) % across) for i in range(across)]
        near = near + lax.ppermute(parts[d], "x", ring)
    pieces = near.reshape(owners // 2 // across, -1, width)
    pieces = jnp.concatenate([pieces, pieces], axis=0)
    pieces = lax.all_to_all(pieces, ("rep", "z", "y_hi"), 0, 0, tiled=True)
    light_sums = light_kernel(recv)
    heavy_sums = jnp.sum(pieces, axis=0)
    return (light_sums, heavy_sums)


def solution(mesh):
    own = ("x", "z", "y_hi", "core")
    every = ("rep",) + own
    mesh = jax.sharding.Mesh(mesh.devices.reshape(2, 4, 4, 2, 2), every)
    placed = (P(every, None), P(every), P(), P(every, None), P(every, None))
    return jax.shard_map(
        per_device,
        mesh=mesh,
        in_specs=placed,
        out_specs=(P(own, None), P(own, None)),
        check_vma=False,
    )
```

```python
import jax
import jax.numpy as jnp
from jax import lax
from jax.experimental import pallas as pl
from jax.experimental.pallas import tpu as pltpu
from jax.sharding import PartitionSpec as P

KEYS_DEV = 4096
CAP = 64
LANES = 128
BANKS = 8
CHUNK = 32
HALF = 32


def pack_blocks(offs, cnts, keys, values, sizes):
    nr, nx, nz, ny, nc = sizes
    events, width = values.shape
    key_rows = events // LANES
    block = CAP + 1
    groups, members = nz * ny, nx * nc
    owners = groups * members

    def owner_of(g, m):
        return (((m // nc) * nz + g // ny) * ny + g % ny) * nc + m % nc

    def body(off_ref, cnt_ref, keys_ref, val_ref, out_ref, rows, buf, krow, arow, last, in_sem, out_sem):
        lane = lax.broadcasted_iota(jnp.int32, (1, LANES), 1)

        load = pltpu.make_async_copy(val_ref, rows, in_sem)
        load.start()

        def block_keys(b, carry):
            o = owner_of(b // members, b % members)
            off = off_ref[0, o]
            end = off + cnt_ref[0, o]
            start = jnp.minimum(off, events - CAP)
            row = start // LANES
            shift = start - row * LANES
            row_next = jnp.minimum(row + 1, key_rows - 1)
            first = lane >= shift
            pos = jnp.where(first, row * LANES + lane, (row + 1) * LANES + lane)
            key = jnp.where(first, keys_ref[pl.ds(row, 1), :], keys_ref[pl.ds(row_next, 1), :])
            inside = (pos >= off) & (pos < end)
            krow[pl.ds(b, 1), :] = jnp.where(inside, key - o * KEYS_DEV, KEYS_DEV)
            arow[pl.ds(b, 1), :] = jnp.full((1, LANES), shift, jnp.int32)
            last[pl.ds(b, 1), :] = jnp.full((1, LANES), end - start, jnp.int32)
            return carry

        lax.fori_loop(0, owners, block_keys, 0, unroll=16)
        rolled = krow[...]
        shifts = arow[...]
        for bit in range(7):
            moved = pltpu.roll(rolled, LANES - (1 << bit), 1)
            rolled = jnp.where((shifts >> bit) & 1 == 1, moved, rolled)
        lanes = lax.broadcasted_iota(jnp.int32, rolled.shape, 1)
        krow[...] = jnp.where(lanes == CAP, last[...], rolled)
        load.wait()
        stores = []
        for g in range(groups):
            for m in range(members):
                b = g * members + m
                start = jnp.minimum(off_ref[0, owner_of(g, m)], events - CAP)
                buf[pl.ds(b * block, CAP), :] = rows[pl.ds(start, CAP), :]
                buf[pl.ds(b * block + CAP, 1), :] = krow[pl.ds(b, 1), :].astype(jnp.float32)
            span = pl.ds(g * members * block, members * block)
            for r in range(nr):
                store = pltpu.make_async_copy(
                    buf.at[span], out_ref.at[g * nr + r], out_sem.at[g * nr + r]
                )
                store.start()
                stores.append(store)
        for store in stores:
            store.wait()

    smem = pl.BlockSpec(memory_space=pltpu.SMEM)
    packed = pl.pallas_call(
        body,
        out_shape=jax.ShapeDtypeStruct((groups * nr, members * block, width), jnp.float32),
        in_specs=[
            smem,
            smem,
            pl.BlockSpec(memory_space=pltpu.VMEM),
            pl.BlockSpec(memory_space=pl.ANY),
        ],
        out_specs=pl.BlockSpec(memory_space=pl.ANY),
        scratch_shapes=[
            pltpu.VMEM((events, width), jnp.float32),
            pltpu.VMEM((owners * block, width), jnp.float32),
            pltpu.VMEM((owners, LANES), jnp.int32),
            pltpu.VMEM((owners, LANES), jnp.int32),
            pltpu.VMEM((owners, LANES), jnp.int32),
            pltpu.SemaphoreType.DMA,
            pltpu.SemaphoreType.DMA((groups * nr,)),
        ],
        name="pack_blocks",
    )(offs, cnts, keys.reshape(key_rows, LANES), values)
    return packed.reshape(nr * owners, block, 1, width)


def light_kernel(recv):
    senders, block, _, width = recv.shape
    chunks = senders // CHUNK

    def body(recv_ref, out_ref, rows, kint, ksm, *rest):
        acc = rest[:BANKS]
        key_sem, smem_sem, row_sems, out_sems = rest[BANKS:]
        key_copy = pltpu.make_async_copy(recv_ref.at[:, CAP], rows.at[:, CAP], key_sem)
        key_copy.start()
        copies = []
        for c in range(chunks):
            part = (pl.ds(c * CHUNK, CHUNK), pl.ds(0, CAP))
            copies.append(
                pltpu.make_async_copy(recv_ref.at[part], rows.at[part], row_sems.at[c])
            )
            copies[c].start()
        zeros = jnp.zeros((64, width), jnp.float32)

        def clear(i, carry):
            for bank in acc:
                bank[pl.ds(i * 64, 64), :] = zeros
            return carry

        def convert(i, longer):
            keys = rows[i, CAP].astype(jnp.int32)
            kint[i] = keys
            return longer + jnp.where(keys > HALF, 1, 0)

        spans = KEYS_DEV // 64
        lax.fori_loop(0, spans * 5 // 8, clear, 0)
        key_copy.wait()
        longer = jnp.zeros((1, width), jnp.int32)
        longer = lax.fori_loop(0, senders, convert, longer, unroll=8)
        smem_copy = pltpu.make_async_copy(kint, ksm, smem_sem)
        smem_copy.start()
        lane = lax.broadcasted_iota(jnp.int32, (1, width), 1)
        full = jnp.sum(jnp.where(lane == CAP, longer, 0)) * 2 > senders
        lax.fori_loop(spans * 5 // 8, spans, clear, 0)
        smem_copy.wait()

        def add_slots(i, slots):
            for s in slots:
                bank = acc[s % BANKS]
                key = ksm[i, 0, s]
                bank[pl.ds(key, 1), :] = bank[pl.ds(key, 1), :] + rows[i, s]

        def sender(i, carry):
            add_slots(i, range(CAP))
            return carry

        def short_sender(i, carry):
            add_slots(i, range(HALF))

            @pl.when(ksm[i, 0, CAP] > HALF)
            def _():
                add_slots(i, range(HALF, CAP))

            return carry

        for c in range(chunks):
            copies[c].wait()

            @pl.when(full)
            def _():
                lax.fori_loop(c * CHUNK, (c + 1) * CHUNK, sender, 0, unroll=4)

            @pl.when(jnp.logical_not(full))
            def _():
                lax.fori_loop(c * CHUNK, (c + 1) * CHUNK, short_sender, 0, unroll=4)


        def finish(i, carry):
            span = pl.ds(i * 64, 64)
            total = acc[0][span, :]
            for bank in acc[1:]:
                total = total + bank[span, :]
            acc[0][span, :] = total
            return carry

        parts = 8
        stores = []
        for c in range(parts):
            step = KEYS_DEV // parts
            lax.fori_loop(c * step // 64, (c + 1) * step // 64, finish, 0)
            span = pl.ds(c * step, step)
            stores.append(pltpu.make_async_copy(acc[0].at[span], out_ref.at[span], out_sems.at[c]))
            stores[c].start()
        for store in stores:
            store.wait()

    return pl.pallas_call(
        body,
        out_shape=jax.ShapeDtypeStruct((KEYS_DEV, width), jnp.float32),
        in_specs=[pl.BlockSpec(memory_space=pl.ANY)],
        out_specs=pl.BlockSpec(memory_space=pl.ANY),
        scratch_shapes=[
            pltpu.VMEM((senders, block, 1, width), jnp.float32),
            pltpu.VMEM((senders, 1, width), jnp.int32),
            pltpu.SMEM((senders, 1, width), jnp.int32),
        ]
        + [pltpu.VMEM((KEYS_DEV + 8, width), jnp.float32) for _ in range(BANKS)]
        + [
            pltpu.SemaphoreType.DMA,
            pltpu.SemaphoreType.DMA,
            pltpu.SemaphoreType.DMA((chunks,)),
            pltpu.SemaphoreType.DMA((8,)),
        ],
        name="light_sums",
    )(recv)


def heavy_kernel(values, keys, heavy_ids, place, owners, across):
    events, width = values.shape
    heavy = heavy_ids.shape[0]
    tile = heavy // 2
    step_events = 2048
    event_rows = events // LANES
    rows = step_events // LANES
    half = owners // 2
    stride = half // across
    piece = heavy // owners

    def body(at_ref, h_ref, k_ref, v_ref, near_ref, far_ref, ids, rhs):
        c = pl.program_id(0)

        @pl.when(c == 0)
        def _():
            for p in range(owners):
                x = (at_ref[0] + p % half // stride) % (half // stride)
                core = (at_ref[1] + p // half) % 2
                source = (x * stride + p % stride) * 2 + core
                column = h_ref[pl.ds(pl.multiple_of(source * piece, piece), piece), :]
                ids[pl.ds(p * piece, piece), :] = jnp.broadcast_to(column, (piece, LANES))

            def split(i, carry):
                span = pl.ds(i * 512, 512)
                v = v_ref[span, :]
                high = v.astype(jnp.bfloat16)
                rhs[span, :width] = high
                rhs[span, width:] = (v - high.astype(jnp.float32)).astype(jnp.bfloat16)
                return carry

            lax.fori_loop(0, events // 512, split, 0)

        h = ids[pl.ds(c * tile, tile), :]
        total = None
        for q in range(events // step_events):
            onehot = jnp.concatenate(
                [
                    jnp.where(h == k_ref[pl.ds(q * rows + j, 1), :], 1.0, 0.0).astype(jnp.bfloat16)
                    for j in range(rows)
                ],
                axis=1,
            )
            added = jnp.dot(
                onehot,
                rhs[pl.ds(q * step_events, step_events), :],
                preferred_element_type=jnp.float32,
            )
            total = added if total is None else total + added

        @pl.when(c == 0)
        def _():
            near_ref[...] = total[:, :width] + total[:, width:]

        @pl.when(c == 1)
        def _():
            far_ref[...] = total[:, :width] + total[:, width:]

    side = jax.ShapeDtypeStruct((tile, width), jnp.float32)
    return pl.pallas_call(
        body,
        grid=(2,),
        out_shape=(side, side),
        in_specs=[
            pl.BlockSpec(memory_space=pltpu.SMEM),
            pl.BlockSpec((heavy, 1), lambda c: (0, 0)),
            pl.BlockSpec((event_rows, LANES), lambda c: (0, 0)),
            pl.BlockSpec((events, width), lambda c: (0, 0)),
        ],
        out_specs=(
            pl.BlockSpec((tile, width), lambda c: (0, 0)),
            pl.BlockSpec((tile, width), lambda c: (0, 0)),
        ),
        scratch_shapes=[
            pltpu.VMEM((heavy, LANES), jnp.int32),
            pltpu.VMEM((events, 2 * width), jnp.bfloat16),
        ],
        name="heavy_sums",
    )(place, heavy_ids.reshape(heavy, 1), keys.reshape(event_rows, LANES), values)


def per_device(values, key_ids, heavy_ids, block_offsets, block_counts):
    own = ("x", "z", "y_hi", "core")
    sizes = tuple(lax.axis_size(axis) for axis in ("rep",) + own)
    owners = lax.axis_size(own)
    packed = pack_blocks(block_offsets, block_counts, key_ids, values, sizes)
    order = ("z", "y_hi", "rep", "x", "core")
    recv = lax.all_to_all(packed, order, split_axis=0, concat_axis=0, tiled=True)
    across = lax.axis_size("x")
    place = jnp.stack([lax.axis_index("x"), lax.axis_index("core")]).astype(jnp.int32)
    near, far = heavy_kernel(values, key_ids, heavy_ids, place, owners, across)
    width = near.shape[1]
    near = near + lax.ppermute(far, "core", [(0, 1), (1, 0)])
    parts = near.reshape(across, -1, width)
    near = parts[0]
    for d in range(1, across):
        ring = [(i, (i + d) % across) for i in range(across)]
        near = near + lax.ppermute(parts[d], "x", ring)
    pieces = near.reshape(owners // 2 // across, -1, width)
    pieces = jnp.concatenate([pieces, pieces], axis=0)
    pieces = lax.all_to_all(pieces, ("rep", "z", "y_hi"), 0, 0, tiled=True)
    light_sums = light_kernel(recv)
    heavy_sums = jnp.sum(pieces, axis=0)
    return (light_sums, heavy_sums)


def solution(mesh):
    own = ("x", "z", "y_hi", "core")
    every = ("rep",) + own
    mesh = jax.sharding.Mesh(mesh.devices.reshape(2, 4, 4, 2, 2), every)
    placed = (P(every, None), P(every), P(), P(every, None), P(every, None))
    return jax.shard_map(
        per_device,
        mesh=mesh,
        in_specs=placed,
        out_specs=(P(own, None), P(own, None)),
        check_vma=False,
    )
```

```python
import jax
import jax.numpy as jnp
from jax import lax
from jax.experimental import pallas as pl
from jax.experimental.pallas import tpu as pltpu
from jax.sharding import PartitionSpec as P

KEYS_DEV = 4096
CAP = 64
LANES = 128
BANKS = 8
CHUNK = 32
HALF = 32


def pack_blocks(offs, cnts, keys, values, sizes):
    nr, nx, nz, ny, nc = sizes
    events, width = values.shape
    key_rows = events // LANES
    block = CAP + 1
    groups, members = nz * ny, nx * nc
    owners = groups * members

    def owner_of(g, m):
        return (((m // nc) * nz + g // ny) * ny + g % ny) * nc + m % nc

    def body(off_ref, cnt_ref, keys_ref, val_ref, out_ref, rows, buf, krow, arow, last, in_sem, out_sem):
        lane = lax.broadcasted_iota(jnp.int32, (1, LANES), 1)

        load = pltpu.make_async_copy(val_ref, rows, in_sem)
        load.start()

        def block_keys(b, carry):
            o = owner_of(b // members, b % members)
            off = off_ref[0, o]
            end = off + cnt_ref[0, o]
            start = jnp.minimum(off, events - CAP)
            row = start // LANES
            shift = start - row * LANES
            row_next = jnp.minimum(row + 1, key_rows - 1)
            first = lane >= shift
            pos = jnp.where(first, row * LANES + lane, (row + 1) * LANES + lane)
            key = jnp.where(first, keys_ref[pl.ds(row, 1), :], keys_ref[pl.ds(row_next, 1), :])
            inside = (pos >= off) & (pos < end)
            krow[pl.ds(b, 1), :] = jnp.where(inside, key - o * KEYS_DEV, KEYS_DEV)
            arow[pl.ds(b, 1), :] = jnp.full((1, LANES), shift, jnp.int32)
            last[pl.ds(b, 1), :] = jnp.full((1, LANES), end - start, jnp.int32)
            return carry

        lax.fori_loop(0, owners, block_keys, 0, unroll=16)
        rolled = krow[...]
        shifts = arow[...]
        for bit in range(7):
            moved = pltpu.roll(rolled, LANES - (1 << bit), 1)
            rolled = jnp.where((shifts >> bit) & 1 == 1, moved, rolled)
        lanes = lax.broadcasted_iota(jnp.int32, rolled.shape, 1)
        krow[...] = jnp.where(lanes == CAP, last[...], rolled)
        load.wait()
        stores = []
        for g in range(groups):
            for m in range(members):
                b = g * members + m
                start = jnp.minimum(off_ref[0, owner_of(g, m)], events - CAP)
                buf[pl.ds(b * block, CAP), :] = rows[pl.ds(start, CAP), :]
                buf[pl.ds(b * block + CAP, 1), :] = krow[pl.ds(b, 1), :].astype(jnp.float32)
            span = pl.ds(g * members * block, members * block)
            for r in range(nr):
                store = pltpu.make_async_copy(
                    buf.at[span], out_ref.at[g * nr + r], out_sem.at[g * nr + r]
                )
                store.start()
                stores.append(store)
        for store in stores:
            store.wait()

    smem = pl.BlockSpec(memory_space=pltpu.SMEM)
    packed = pl.pallas_call(
        body,
        out_shape=jax.ShapeDtypeStruct((groups * nr, members * block, width), jnp.float32),
        in_specs=[
            smem,
            smem,
            pl.BlockSpec(memory_space=pltpu.VMEM),
            pl.BlockSpec(memory_space=pl.ANY),
        ],
        out_specs=pl.BlockSpec(memory_space=pl.ANY),
        scratch_shapes=[
            pltpu.VMEM((events, width), jnp.float32),
            pltpu.VMEM((owners * block, width), jnp.float32),
            pltpu.VMEM((owners, LANES), jnp.int32),
            pltpu.VMEM((owners, LANES), jnp.int32),
            pltpu.VMEM((owners, LANES), jnp.int32),
            pltpu.SemaphoreType.DMA,
            pltpu.SemaphoreType.DMA((groups * nr,)),
        ],
        name="pack_blocks",
    )(offs, cnts, keys.reshape(key_rows, LANES), values)
    return packed.reshape(nr * owners, block, 1, width)


def light_kernel(recv):
    senders, block, _, width = recv.shape
    chunks = senders // CHUNK

    def body(recv_ref, out_ref, rows, kint, ksm, *rest):
        acc = rest[:BANKS]
        key_sem, smem_sem, row_sems, out_sems = rest[BANKS:]
        key_copy = pltpu.make_async_copy(recv_ref.at[:, CAP], rows.at[:, CAP], key_sem)
        key_copy.start()
        copies = []
        for c in range(chunks):
            part = (pl.ds(c * CHUNK, CHUNK), pl.ds(0, CAP))
            copies.append(
                pltpu.make_async_copy(recv_ref.at[part], rows.at[part], row_sems.at[c])
            )
            copies[c].start()
        zeros = jnp.zeros((64, width), jnp.float32)

        def clear(i, carry):
            for bank in acc:
                bank[pl.ds(i * 64, 64), :] = zeros
            return carry

        def convert(i, longer):
            keys = rows[i, CAP].astype(jnp.int32)
            kint[i] = keys
            return longer + jnp.where(keys > HALF, 1, 0)

        spans = KEYS_DEV // 64
        lax.fori_loop(0, spans * 5 // 8, clear, 0)
        key_copy.wait()
        longer = jnp.zeros((1, width), jnp.int32)
        longer = lax.fori_loop(0, senders, convert, longer, unroll=8)
        smem_copy = pltpu.make_async_copy(kint, ksm, smem_sem)
        smem_copy.start()
        lane = lax.broadcasted_iota(jnp.int32, (1, width), 1)
        full = jnp.sum(jnp.where(lane == CAP, longer, 0)) * 2 > senders
        lax.fori_loop(spans * 5 // 8, spans, clear, 0)
        smem_copy.wait()

        def add_slots(i, slots):
            for s in slots:
                bank = acc[s % BANKS]
                key = ksm[i, 0, s]
                bank[pl.ds(key, 1), :] = bank[pl.ds(key, 1), :] + rows[i, s]

        def sender(i, carry):
            add_slots(i, range(CAP))
            return carry

        def short_sender(i, carry):
            add_slots(i, range(HALF))

            @pl.when(ksm[i, 0, CAP] > HALF)
            def _():
                add_slots(i, range(HALF, CAP))

            return carry

        for c in range(chunks):
            copies[c].wait()

            @pl.when(full)
            def _():
                lax.fori_loop(c * CHUNK, (c + 1) * CHUNK, sender, 0, unroll=4)

            @pl.when(jnp.logical_not(full))
            def _():
                lax.fori_loop(c * CHUNK, (c + 1) * CHUNK, short_sender, 0, unroll=8)


        def finish(i, carry):
            span = pl.ds(i * 64, 64)
            total = acc[0][span, :]
            for bank in acc[1:]:
                total = total + bank[span, :]
            acc[0][span, :] = total
            return carry

        parts = 8
        stores = []
        for c in range(parts):
            step = KEYS_DEV // parts
            lax.fori_loop(c * step // 64, (c + 1) * step // 64, finish, 0)
            span = pl.ds(c * step, step)
            stores.append(pltpu.make_async_copy(acc[0].at[span], out_ref.at[span], out_sems.at[c]))
            stores[c].start()
        for store in stores:
            store.wait()

    return pl.pallas_call(
        body,
        out_shape=jax.ShapeDtypeStruct((KEYS_DEV, width), jnp.float32),
        in_specs=[pl.BlockSpec(memory_space=pl.ANY)],
        out_specs=pl.BlockSpec(memory_space=pl.ANY),
        scratch_shapes=[
            pltpu.VMEM((senders, block, 1, width), jnp.float32),
            pltpu.VMEM((senders, 1, width), jnp.int32),
            pltpu.SMEM((senders, 1, width), jnp.int32),
        ]
        + [pltpu.VMEM((KEYS_DEV + 8, width), jnp.float32) for _ in range(BANKS)]
        + [
            pltpu.SemaphoreType.DMA,
            pltpu.SemaphoreType.DMA,
            pltpu.SemaphoreType.DMA((chunks,)),
            pltpu.SemaphoreType.DMA((8,)),
        ],
        name="light_sums",
    )(recv)


def heavy_kernel(values, keys, heavy_ids, place, owners, across):
    events, width = values.shape
    heavy = heavy_ids.shape[0]
    tile = heavy // 2
    step_events = 2048
    event_rows = events // LANES
    rows = step_events // LANES
    half = owners // 2
    stride = half // across
    piece = heavy // owners

    def body(at_ref, h_ref, k_ref, v_ref, near_ref, far_ref, ids, rhs):
        c = pl.program_id(0)

        @pl.when(c == 0)
        def _():
            for p in range(owners):
                x = (at_ref[0] + p % half // stride) % (half // stride)
                core = (at_ref[1] + p // half) % 2
                source = (x * stride + p % stride) * 2 + core
                column = h_ref[pl.ds(pl.multiple_of(source * piece, piece), piece), :]
                ids[pl.ds(p * piece, piece), :] = jnp.broadcast_to(column, (piece, LANES))

            def split(i, carry):
                span = pl.ds(i * 512, 512)
                v = v_ref[span, :]
                high = v.astype(jnp.bfloat16)
                rhs[span, :width] = high
                rhs[span, width:] = (v - high.astype(jnp.float32)).astype(jnp.bfloat16)
                return carry

            lax.fori_loop(0, events // 512, split, 0)

        h = ids[pl.ds(c * tile, tile), :]
        total = None
        for q in range(events // step_events):
            onehot = jnp.concatenate(
                [
                    jnp.where(h == k_ref[pl.ds(q * rows + j, 1), :], 1.0, 0.0).astype(jnp.bfloat16)
                    for j in range(rows)
                ],
                axis=1,
            )
            added = jnp.dot(
                onehot,
                rhs[pl.ds(q * step_events, step_events), :],
                preferred_element_type=jnp.float32,
            )
            total = added if total is None else total + added

        @pl.when(c == 0)
        def _():
            near_ref[...] = total[:, :width] + total[:, width:]

        @pl.when(c == 1)
        def _():
            far_ref[...] = total[:, :width] + total[:, width:]

    side = jax.ShapeDtypeStruct((tile, width), jnp.float32)
    return pl.pallas_call(
        body,
        grid=(2,),
        out_shape=(side, side),
        in_specs=[
            pl.BlockSpec(memory_space=pltpu.SMEM),
            pl.BlockSpec((heavy, 1), lambda c: (0, 0)),
            pl.BlockSpec((event_rows, LANES), lambda c: (0, 0)),
            pl.BlockSpec((events, width), lambda c: (0, 0)),
        ],
        out_specs=(
            pl.BlockSpec((tile, width), lambda c: (0, 0)),
            pl.BlockSpec((tile, width), lambda c: (0, 0)),
        ),
        scratch_shapes=[
            pltpu.VMEM((heavy, LANES), jnp.int32),
            pltpu.VMEM((events, 2 * width), jnp.bfloat16),
        ],
        name="heavy_sums",
    )(place, heavy_ids.reshape(heavy, 1), keys.reshape(event_rows, LANES), values)


def sum_twice(*parts):
    count = parts[0].shape[0]

    def body(*refs):
        total = refs[0][...]
        for ref in refs[1:-1]:
            total = total + ref[...]
        refs[-1][:count] = total
        refs[-1][count:] = total

    vmem = pl.BlockSpec(memory_space=pltpu.VMEM)
    return pl.pallas_call(
        body,
        out_shape=jax.ShapeDtypeStruct((2 * count,) + parts[0].shape[1:], jnp.float32),
        in_specs=[vmem] * len(parts),
        out_specs=vmem,
        compiler_params=pltpu.CompilerParams(vmem_limit_bytes=4 << 20),
        name="sum_twice",
    )(*parts)


def per_device(values, key_ids, heavy_ids, block_offsets, block_counts):
    own = ("x", "z", "y_hi", "core")
    sizes = tuple(lax.axis_size(axis) for axis in ("rep",) + own)
    owners = lax.axis_size(own)
    packed = pack_blocks(block_offsets, block_counts, key_ids, values, sizes)
    order = ("z", "y_hi", "rep", "x", "core")
    recv = lax.all_to_all(packed, order, split_axis=0, concat_axis=0, tiled=True)
    across = lax.axis_size("x")
    place = jnp.stack([lax.axis_index("x"), lax.axis_index("core")]).astype(jnp.int32)
    near, far = heavy_kernel(values, key_ids, heavy_ids, place, owners, across)
    width = near.shape[1]
    near = near + lax.ppermute(far, "core", [(0, 1), (1, 0)])
    parts = near.reshape(across, owners // 2 // across, -1, width)
    sent = []
    for d in range(1, across):
        ring = [(i, (i + d) % across) for i in range(across)]
        sent.append(lax.ppermute(parts[d], "x", ring))
    pieces = sum_twice(parts[0], *sent)
    pieces = lax.all_to_all(pieces, ("rep", "z", "y_hi"), 0, 0, tiled=True)
    light_sums = light_kernel(recv)
    heavy_sums = jnp.sum(pieces, axis=0)
    return (light_sums, heavy_sums)


def solution(mesh):
    own = ("x", "z", "y_hi", "core")
    every = ("rep",) + own
    mesh = jax.sharding.Mesh(mesh.devices.reshape(2, 4, 4, 2, 2), every)
    placed = (P(every, None), P(every), P(), P(every, None), P(every, None))
    return jax.shard_map(
        per_device,
        mesh=mesh,
        in_specs=placed,
        out_specs=(P(own, None), P(own, None)),
        check_vma=False,
    )
```
